32 devices in a mesh: zero: 4 (over y, x), width: 8 (over z, core).
Axes of the slice: x: 2, y: 2, z: 4, core: 2. Of those that a mesh axis runs over, the one named last changes fastest.
Arguments:
- train_gate: float32 [5120, 13824], P('zero', 'width'), may hold values from -0.125 to 0.125
- drift_gate: float32 [5120, 13824], P('zero', 'width'), may hold values from -0.078125 to 0.078125
- spread_gate: float32 [5120, 13824], P('zero', 'width'), may hold values from -0.078125 to 0.078125
- train_up: float32 [5120, 13824], P('zero', 'width'), may hold values from -0.125 to 0.125
- drift_up: float32 [5120, 13824], P('zero', 'width'), may hold values from -0.078125 to 0.078125
- spread_up: float32 [5120, 13824], P('zero', 'width'), may hold values from -0.078125 to 0.078125
- norm_gain: float32 [5120], P('zero'), may hold values from 0.25 to 1.75
Outputs:
- serving_gate: bfloat16 [5120, 13824], P(None, 'width')
- serving_up: bfloat16 [5120, 13824], P(None, 'width')
- factor_gate: float32 [13824], P('width')
- factor_up: float32 [13824], P('width')
The draws below stay inside these ranges and needn't reach their ends.
All inputs are finite; a program needn't handle non-finite values. Where the reference program divides by a largest or mean magnitude, that divisor is 1e-20 or more.
Results may differ from the reference program's by a relative error of at most 0.001.
Values may be sent and summed in bfloat16 or wider, within the bound.
A program may use at most 192 MiB of HBM per device.

```python
import jax
import jax.numpy as jnp

D_MODEL = 5120
D_INNER = 13824


def spiked(values, key, source, target, blocks, factor):
    def block_of(axis_at):
        return (jnp.arange(values.shape[axis_at]) // (values.shape[axis_at] // blocks)).reshape((-1,) + (1,) * (values.ndim - 1 - axis_at))

    one_side = jax.random.permutation(key, blocks)[block_of(target)]
    second = (block_of(target) + blocks // 2) % blocks
    return jnp.where((block_of(source) == one_side) | (block_of(source) == second), factor * values, values)


def block_scale(key, dims, cuts, least, high):
    gain, own = 1.0, jax.random.fold_in(key, 6)
    for axis_at, blocks in cuts:
        steps = jnp.exp(jax.random.uniform(jax.random.fold_in(own, axis_at), (blocks,), jnp.float32, least / len(cuts), high / len(cuts)))
        gain = gain * jnp.repeat(steps, dims[axis_at] // blocks).reshape([-1 if axis == axis_at else 1 for axis in range(len(dims))])
    return gain


def normal_values(rng, extent, width, bound, cuts=(), kind=jnp.bfloat16):
    result = jax.random.normal(rng, extent, jnp.float32) * width
    if len(cuts) > 0:
        result = block_scale(rng, extent, cuts, -0.22, 0.18) * result
    return jnp.clip(result, min=-bound, max=bound).astype(kind)


def heavy_noise(own_key, dims, deviation, bound, cuts, heavy, held_as=jnp.bfloat16):
    array = deviation * jax.random.normal(own_key, dims, jnp.float32)
    if cuts:
        array = array * block_scale(own_key, dims, cuts, -0.22, 0.18)
    return jnp.clip(spiked(array, jax.random.fold_in(own_key, 3), *heavy), -bound, bound).astype(held_as)


def setup_inputs(seed: int = 0) -> dict:
    arg_keys = jax.random.split(jax.random.key(seed), 8)
    return {
        "train_gate": heavy_noise(arg_keys[0], (D_MODEL, D_INNER), D_MODEL ** -0.5, 0.125, ((0, 4), (1, 8)), (0, 1, 8, 2.0), jnp.float32),
        "drift_gate": normal_values(arg_keys[1], (D_MODEL, D_INNER), D_MODEL ** -0.5, 0.078125, ((0, 4), (1, 8)), jnp.float32),
        "spread_gate": normal_values(arg_keys[2], (D_MODEL, D_INNER), D_MODEL ** -0.5, 0.078125, ((0, 4), (1, 8)), jnp.float32),
        "train_up": heavy_noise(arg_keys[3], (D_MODEL, D_INNER), D_MODEL ** -0.5, 0.125, ((0, 4), (1, 8)), (0, 1, 8, 2.0), jnp.float32),
        "drift_up": normal_values(arg_keys[4], (D_MODEL, D_INNER), D_MODEL ** -0.5, 0.078125, ((0, 4), (1, 8)), jnp.float32),
        "spread_up": normal_values(arg_keys[5], (D_MODEL, D_INNER), D_MODEL ** -0.5, 0.078125, ((0, 4), (1, 8)), jnp.float32),
        "norm_gain": jnp.clip(1.0 + 0.15 * jax.random.normal(arg_keys[6], (D_MODEL,), jnp.float32), 0.25, 1.75),
    }


learn_rate = 0.3
hold_rate = 0.9


def reference(train_gate, drift_gate, spread_gate, train_up, drift_up, spread_up, norm_gain):
    hold_gate = hold_rate * drift_gate + spread_gate
    whole_gate = train_gate - learn_rate * hold_gate
    hold_up = hold_rate * drift_up + spread_up
    whole_up = train_up - learn_rate * hold_up
    whole_gained_gate = whole_gate * norm_gain[:, None]
    whole_gained_up = whole_up * norm_gain[:, None]
    factor_gate = jnp.max(jnp.abs(whole_gained_gate), axis=0)
    serving_gate = (whole_gained_gate / factor_gate).astype(jnp.bfloat16)
    factor_up = jnp.max(jnp.abs(whole_gained_up), axis=0)
    serving_up = (whole_gained_up / factor_up).astype(jnp.bfloat16)
    return serving_gate, serving_up, factor_gate, factor_up
```

```python
import jax
import jax.numpy as jnp
from jax import lax
from jax.experimental import pallas as pl
from jax.sharding import PartitionSpec as P


learn_rate = 0.3
hold_rate = 0.9
GATES = (5, 4, 6, 5)
LEADS = 2
UPS = (6, 6, 4, 2, 1)
unit = 8


def cuts_of(width, shares):
    edges, done = [0], 0
    for share in shares[:-1]:
        done += share
        edge = int(done / sum(shares) * width) // unit * unit
        if edges[-1] < edge < width:
            edges.append(edge)
    return list(zip(edges, edges[1:] + [width]))


def gained(train, drift, spread, gain, lo, hi):
    train, drift, spread = train[:, lo:hi], drift[:, lo:hi], spread[:, lo:hi]
    return (train - learn_rate * (hold_rate * drift + spread)) * gain[:, None]


def blank(*shape):
    return pl.pallas_call(
        lambda *refs: None,
        out_shape=[jax.ShapeDtypeStruct(shape, jnp.bfloat16)] * 2,
        out_specs=[pl.BlockSpec(memory_space=pl.ANY)] * 2,
    )()


def body_of(parts):
    def gather(narrow, out, lo):
        rows = narrow.shape[0]
        me = lax.axis_index("zero")

        def put(out, piece, owner, row=0):
            return lax.dynamic_update_slice(out, piece, (owner * rows + row, jnp.int32(lo)))

        if parts != 4:
            return lax.dynamic_update_slice(out, lax.all_gather(narrow, "zero", axis=0, tiled=True), (0, lo))

        def along(piece, side):
            return lax.ppermute(piece, "zero", [(i, i ^ side) for i in range(parts)])

        half = rows // 2
        first, second = along(narrow, 1), along(narrow, 2)
        far_top, far_bottom = along(first[:half], 2), along(second[half:], 1)
        out = put(out, narrow, me)
        out = put(out, first, me ^ 1)
        out = put(out, second, me ^ 2)
        out = put(out, far_top, me ^ 3)
        return put(out, far_bottom, me ^ 3, half)

    def largest(peaks):
        if parts != 4:
            return lax.pmax(peaks, "zero")
        sizes = [peak.shape[0] for peak in peaks]
        own = every = jnp.concatenate(peaks)
        for side in (1, 2, 3):
            other = lax.ppermute(own, "zero", [(i, i ^ side) for i in range(parts)])
            every = jnp.maximum(every, other)
        return [every[sum(sizes[:k]) : sum(sizes[: k + 1])] for k in range(len(sizes))]

    def body(train_gate, drift_gate, spread_gate, train_up, drift_up, spread_up, norm_gain):
        rows, width = train_gate.shape
        gate, up = (train_gate, drift_gate, spread_gate), (train_up, drift_up, spread_up)
        peak = lambda piece: jnp.max(jnp.abs(piece), axis=0)
        cuts = (cuts_of(width, GATES), cuts_of(width, UPS))
        lead = cuts[0][LEADS - 1][1]
        piece = gained(*gate, norm_gain, 0, lead)
        (factor_lead,) = largest((peak(piece),))
        narrow_lead = (piece / factor_lead).astype(jnp.bfloat16)
        *gate, token = lax.optimization_barrier((*gate, narrow_lead))
        *up, narrow_lead = lax.optimization_barrier((*up, token))
        rest_gate, rest_up = gained(*gate, norm_gain, lead, width), gained(*up, norm_gain, 0, width)
        factor_rest, factor_up = largest((peak(rest_gate), peak(rest_up)))
        scaled = lambda rest, factor, lo, hi: (rest[:, lo:hi] / factor[lo:hi]).astype(jnp.bfloat16)
        early = [narrow_lead[:, lo:hi] for lo, hi in cuts[0][:LEADS]]
        late = [scaled(rest_gate, factor_rest, lo - lead, hi - lead) for lo, hi in cuts[0][LEADS:]]
        late += [scaled(rest_up, factor_up, lo, hi) for lo, hi in cuts[1]]
        pieces = [*lax.optimization_barrier(early), *lax.optimization_barrier(late)]
        outs, turn = [], 0
        for ranges, out in zip(cuts, blank(width, rows * parts)):
            out = out.T
            for lo, _ in ranges:
                out = gather(pieces[turn], out, lo)
                turn += 1
            outs.append(out)
        factor_gate = jnp.concatenate([factor_lead, factor_rest])
        return (*outs, factor_gate, factor_up)

    return body


def solution(mesh):
    return jax.shard_map(
        body_of(mesh.shape["zero"]),
        mesh=mesh,
        in_specs=(
            P("zero", "width"),
            P("zero", "width"),
            P("zero", "width"),
            P("zero", "width"),
            P("zero", "width"),
            P("zero", "width"),
            P("zero"),
        ),
        out_specs=(P(None, "width"), P(None, "width"), P("width"), P("width")),
        check_vma=False,
    )
```
